128 devices in a mesh: row: 4 (over x), col: 4 (over y_lo, core), layer: 8 (over y_hi, z).
Axes of the slice: x: 4, y: 4 (y_hi: 2, y_lo: 2; y = y_hi * 2 + y_lo), z: 4, core: 2. Of those that a mesh axis runs over, the one named last changes fastest.
Arguments:
- left_factor: float32 [6144, 8192], P('row', 'col'), may hold values from -6 to 6
- right_factor: float32 [8192, 6144], P('row', 'col'), may hold values from -0.0625 to 0.0625
Outputs:
- product: float32 [6144, 6144], P(('row', 'layer'), 'col')
The draws below stay inside these ranges and needn't reach their ends.
All inputs are finite; a program needn't handle non-finite values.
Results may differ from the reference program's by a relative error of at most 0.000073.
Values sent between devices are 32-bit elements; how exact they have to be, the bound alone decides.
No kernel may reach another device: no remote copies, remote signals or barrier semaphores. Data moves between devices by JAX's collectives and lax.ppermute only.
A program may use at most 192 MiB of HBM per device.

```python
import jax
import jax.numpy as jnp
from jax import lax

K = 8192
M = 6144
NC = 6144


def spiked(drawn, stream_key, source, target, blocks, factor):
    def block_of(dim):
        return (jnp.arange(drawn.shape[dim]) // (drawn.shape[dim] // blocks)).reshape((-1,) + (1,) * (drawn.ndim - 1 - dim))

    one_side = jax.random.permutation(stream_key, blocks)[block_of(target)]
    second = (block_of(target) + blocks // 2) % blocks
    return jnp.where((block_of(source) == one_side) | (block_of(source) == second), factor * drawn, drawn)


def block_scale(rng, dims, split, least, top_value):
    gain = 1.0
    for position, shards_of in split:
        draws = jax.random.uniform(jax.random.fold_in(jax.random.fold_in(rng, 6), position), (shards_of,), jnp.float32, least / len(split), top_value / len(split))
        gain = gain * jnp.repeat(jnp.exp(draws), dims[position] // shards_of).reshape((-1,) + (1,) * (len(dims) - 1 - position))
    return gain


def gaussian(key, dims, scale, reach, pieces=(), held_as=jnp.bfloat16):
    drawn = scale * jax.random.normal(key, dims, jnp.float32)
    if pieces:
        drawn = drawn * block_scale(key, dims, pieces, -0.22, 0.18)
    return jnp.clip(drawn, -reach, reach).astype(held_as)


def noise_with(key, dims, spread, most, cuts, heavy, dtype=jnp.bfloat16):
    drawn = spread * jax.random.normal(key, dims, jnp.float32)
    if cuts:
        drawn = drawn * block_scale(key, dims, cuts, -0.22, 0.18)
    return jnp.clip(spiked(drawn, jax.random.fold_in(key, 3), *heavy), -most, most).astype(dtype)


def setup_inputs(seed: int = 0) -> dict:
    seeds = jax.random.split(jax.random.key(seed), 3)
    return {
        "left_factor": noise_with(seeds[0], (M, K), 1.0, 6.0, ((0, 4), (1, 4)), (1, 0, 4, 2.0), jnp.float32),
        "right_factor": gaussian(seeds[1], (K, NC), K ** -0.5, 0.0625, ((0, 4), (1, 4)), jnp.float32),
    }


def reference(left_factor, right_factor):
    return jnp.dot(left_factor, right_factor, precision=lax.Precision.HIGHEST, preferred_element_type=jnp.float32)
```

```python
import jax
import jax.numpy as jnp
from jax import lax
from jax.sharding import PartitionSpec as P


AXES = ("row", "col", "layer")


def per_device(left_factor, right_factor):
    rows, cols, layers = (lax.axis_size(name) for name in AXES)
    x, c, l = (lax.axis_index(name) for name in AXES)
    chunk = left_factor.shape[0] // layers
    quarter = chunk // cols
    half = chunk // 2

    def send(value, target):
        pairs = []
        for i in range(rows):
            for j in range(cols):
                for k in range(layers):
                    a, b, d = target(i, j, k)
                    pairs.append(((i * cols + j) * layers + k, (a * cols + b) * layers + d))
        return lax.ppermute(value, AXES, pairs)

    def to_row(shift):
        return lambda i, j, k: ((i + shift) % rows, j, k)

    def take(layer, block):
        start = layer * chunk + block * quarter
        return lax.dynamic_slice_in_dim(left_factor, start, quarter, 0)

    spread = [
        take(l, c),
        send(take(l, c ^ 1), lambda i, j, k: (i, j ^ 1, k)),
        send(take(l, c ^ 2), lambda i, j, k: (i, j ^ 2, k)),
        send(take(l ^ 4, c ^ 3), lambda i, j, k: (i, j ^ 3, k ^ 4)),
    ]

    partial = {}

    def gather(s):
        mine = lax.select_n(((x + s) % rows) ^ c, *spread)
        if s:
            mine = send(mine, to_row(s))
        across = send(mine, lambda i, j, k: (i, j ^ 2, k))
        beside = send(mine, lambda i, j, k: (i, j ^ 1, k))
        far = send(across, lambda i, j, k: (i, j ^ 1, k))
        return [mine, beside, across, far]

    def multiply(pieces):
        return jnp.dot(
            jnp.concatenate(pieces, 0),
            right_factor,
            precision=lax.Precision.HIGH,
            preferred_element_type=jnp.float32,
        )

    opposite = multiply(gather(2))
    both = multiply(gather(3) + gather(1))
    up, down = both[:chunk], both[chunk:]
    own = multiply(gather(0))

    first_up = send(opposite[:half], to_row(1))
    first_down = send(opposite[half:], to_row(-1))
    plain_up = send(up[half:], to_row(1))
    plain_down = send(down[:half], to_row(-1))
    summed_up = send(up[:half] + first_up, to_row(1))
    summed_down = send(down[half:] + first_down, to_row(-1))
    total = jnp.concatenate(
        [own[:half] + summed_up + plain_down, own[half:] + plain_up + summed_down], 0
    )
    total = total.reshape(2, 2, quarter, -1)
    total = jnp.where(c % 2 == 1, total[:, ::-1], total)
    total = jnp.where(c // 2 == 1, total[::-1], total)
    return total.reshape(chunk, -1)


def solution(mesh):
    placed = (P("row", "col"), P("row", "col"))
    return jax.shard_map(
        per_device,
        mesh=mesh,
        in_specs=placed,
        out_specs=P(("row", "layer"), "col"),
        check_vma=False,
    )
```

```python
import functools

import jax
import jax.numpy as jnp
from jax import lax
from jax.experimental import pallas as pl
from jax.experimental.pallas import tpu as pltpu
from jax.sharding import PartitionSpec as P


AXES = ("row", "col", "layer")
BLOCK = 256
VMEM = pl.BlockSpec(memory_space=pltpu.VMEM)


def split(value):
    high = value.astype(jnp.bfloat16)
    return high, (value - high.astype(jnp.float32)).astype(jnp.bfloat16)


def prepare_kernel(b_ref, high_ref, low_ref):
    size = b_ref.shape[0]
    at = pl.ds(pl.program_id(0) * size, size)
    high_ref[at, :], low_ref[at, :] = split(b_ref[...])


def prepare(b):
    depth, width = b.shape
    return pl.pallas_call(
        prepare_kernel,
        grid=(depth // BLOCK,),
        in_specs=[pl.BlockSpec((BLOCK, width), lambda i: (i, 0))],
        out_specs=[VMEM, VMEM],
        out_shape=[pltpu.VMEM(b.shape, jnp.bfloat16)] * 2,
        compiler_params=pltpu.CompilerParams(vmem_limit_bytes=16 << 20),
        name="prepare",
    )(pltpu.with_memory_space_constraint(b, pltpu.HBM))


def multiply_kernel(count, *refs):
    pieces, (high_ref, low_ref), outs = refs[:count], refs[count : count + 2], refs[count + 2 :]
    high, low = split(jnp.concatenate([piece[...] for piece in pieces], 0))
    dot = functools.partial(jnp.dot, preferred_element_type=jnp.float32)
    size = pieces[0].shape[0]
    for start in range(0, high_ref.shape[1], BLOCK):
        at = slice(start, start + BLOCK)
        result = dot(high, high_ref[:, at]) + dot(high, low_ref[:, at]) + dot(low, high_ref[:, at])
        for i, out in enumerate(outs):
            out[:, at] = result[i * size : (i + 1) * size]


def multiply(pieces, b_high, b_low):
    pieces = [pltpu.with_memory_space_constraint(v, pltpu.VMEM) for v in pieces]
    (size, depth), width = pieces[0].shape, b_high.shape[1]
    rows = size * len(pieces)
    return pl.pallas_call(
        functools.partial(multiply_kernel, len(pieces)),
        in_specs=[VMEM] * (len(pieces) + 2),
        out_specs=[VMEM] * len(pieces),
        out_shape=[pltpu.VMEM((size, width), jnp.float32)] * len(pieces),
        compiler_params=pltpu.CompilerParams(vmem_limit_bytes=16 << 20),
        cost_estimate=pl.CostEstimate(
            flops=6 * rows * depth * width, bytes_accessed=4 * rows * depth, transcendentals=0
        ),
    )(*pieces, b_high, b_low)


def after(values, anchors):
    return lax.optimization_barrier((tuple(values), tuple(anchors)))[0]


def per_device(left_factor, right_factor):
    rows, cols, layers = (lax.axis_size(name) for name in AXES)
    x, c, l = (lax.axis_index(name) for name in AXES)
    chunk = left_factor.shape[0] // layers
    quarter = chunk // cols

    def send(value, target):
        pairs = []
        for i in range(rows):
            for j in range(cols):
                for k in range(layers):
                    a, b, d = target(i, j, k)
                    pairs.append(((i * cols + j) * layers + k, (a * cols + b) * layers + d))
        return lax.ppermute(value, AXES, pairs)

    def to_row(shift):
        return lambda i, j, k: ((i + shift) % rows, j, k)

    def over_y(i, j, k):
        return i, j ^ 2, k

    def over_core(i, j, k):
        return i, j ^ 1, k

    def take(layer, block):
        start = layer * chunk + block * quarter
        return lax.dynamic_slice_in_dim(left_factor, start, quarter, 0)

    b_high, b_low = prepare(right_factor)
    mul = lambda pieces: multiply(pieces, b_high, b_low)

    spread = [
        take(l, c),
        send(take(l, c ^ 1), over_core),
        send(take(l, c ^ 2), over_y),
        send(take(l ^ 4, c ^ 3), lambda i, j, k: (i, j ^ 3, k ^ 4)),
    ]
    swap_core, swap_y = c % 2 == 1, c // 2 == 1
    swap_core, swap_y, *spread = lax.optimization_barrier((swap_core, swap_y, *spread))
    pick = lambda s: lax.select_n(((x + s) % rows) ^ c, *spread)

    mine2 = send(pick(2), to_row(2))
    mine3 = send(pick(3), to_row(3))
    mine1 = send(pick(1), to_row(1))
    mine0 = pick(0)
    across0 = send(mine0, over_y)
    across2 = send(mine2, over_y)
    near2 = send(mine2, over_core)
    opposite_e = mul([mine2, near2])
    first_up_e = send(opposite_e[0], to_row(1))
    first_down_e = send(opposite_e[1], to_row(-1))

    mine3, mine1 = after((mine3, mine1), opposite_e)
    across3 = send(mine3, over_y)
    near3 = send(mine3, over_core)
    across1 = send(mine1, over_y)
    near1 = send(mine1, over_core)
    both_e = mul([mine3, near3, mine1, near1])
    up_e = jnp.concatenate([both_e[0] + first_up_e, both_e[1]], 0)
    down_e = jnp.concatenate([both_e[2], both_e[3] + first_down_e], 0)
    up_e = send(up_e, to_row(1))
    down_e = send(down_e, to_row(-1))

    (across2,) = after((across2,), both_e)
    far2 = send(across2, over_core)
    opposite_l = mul([across2, far2])
    first_up_l = send(opposite_l[0], to_row(1))
    first_down_l = send(opposite_l[1], to_row(-1))

    across3, across1 = after((across3, across1), opposite_l)
    far3 = send(across3, over_core)
    far1 = send(across1, over_core)
    both_l = mul([across3, far3, across1, far1])
    up_l = jnp.concatenate([both_l[0] + first_up_l, both_l[1]], 0)
    down_l = jnp.concatenate([both_l[2], both_l[3] + first_down_l], 0)

    mine0, across0 = after((mine0, across0), both_l)
    near0 = send(mine0, over_core)
    far0 = send(across0, over_core)
    own = mul([mine0, near0, across0, far0])

    up_l = send(up_l, to_row(1))
    down_l = send(down_l, to_row(-1))

    total_e = jnp.concatenate(own[:2], 0) + up_e + down_e
    total_l = jnp.concatenate(own[2:], 0) + up_l + down_l
    total = jnp.stack([total_e, total_l]).reshape(2, 2, quarter, -1)
    total = jnp.where(swap_core, total[:, ::-1], total)
    total = jnp.where(swap_y, total[::-1], total)
    return total.reshape(chunk, -1)


def solution(mesh):
    placed = (P("row", "col"), P("row", "col"))

    return jax.shard_map(
        per_device,
        mesh=mesh,
        in_specs=placed,
        out_specs=P(("row", "layer"), "col"),
        check_vma=False,
    )
```

```python
import functools

import jax
import jax.numpy as jnp
from jax import lax
from jax.experimental import pallas as pl
from jax.experimental.pallas import tpu as pltpu
from jax.sharding import PartitionSpec as P


AXES = ("row", "col", "layer")
BLOCK = 256
VMEM = pl.BlockSpec(memory_space=pltpu.VMEM)


def split(value):
    high = value.astype(jnp.bfloat16)
    return high, (value - high.astype(jnp.float32)).astype(jnp.bfloat16)


def prepare_kernel(b_ref, high_ref, low_ref):
    size = b_ref.shape[0]
    at = pl.ds(pl.program_id(0) * size, size)
    high_ref[at, :], low_ref[at, :] = split(b_ref[...])


def prepare(b):
    depth, width = b.shape
    return pl.pallas_call(
        prepare_kernel,
        grid=(depth // BLOCK,),
        in_specs=[pl.BlockSpec((BLOCK, width), lambda i: (i, 0))],
        out_specs=[VMEM, VMEM],
        out_shape=[pltpu.VMEM(b.shape, jnp.bfloat16)] * 2,
        compiler_params=pltpu.CompilerParams(vmem_limit_bytes=16 << 20),
        name="prepare",
    )(pltpu.with_memory_space_constraint(b, pltpu.HBM))


def multiply_kernel(count, *refs):
    pieces, (high_ref, low_ref), outs = refs[:count], refs[count : count + 2], refs[count + 2 :]
    high, low = split(jnp.concatenate([piece[...] for piece in pieces], 0))
    dot = functools.partial(jnp.dot, preferred_element_type=jnp.float32)
    size = outs[0].shape[0]
    for start in range(0, high_ref.shape[1], BLOCK):
        at = slice(start, start + BLOCK)
        result = dot(high, high_ref[:, at]) + dot(high, low_ref[:, at]) + dot(low, high_ref[:, at])
        for i, out in enumerate(outs):
            out[:, at] = result[i * size : (i + 1) * size]


def in_vmem(values):
    return [pltpu.with_memory_space_constraint(v, pltpu.VMEM) for v in values]


def multiply(pieces, b_high, b_low):
    (size, depth), width = pieces[0].shape, b_high.shape[1]
    rows, results = size * len(pieces), len(pieces) // 2
    return pl.pallas_call(
        functools.partial(multiply_kernel, len(pieces)),
        in_specs=[VMEM] * (len(pieces) + 2),
        out_specs=[VMEM] * results,
        out_shape=[pltpu.VMEM((2 * size, width), jnp.float32)] * results,
        compiler_params=pltpu.CompilerParams(vmem_limit_bytes=16 << 20),
        cost_estimate=pl.CostEstimate(
            flops=6 * rows * depth * width, bytes_accessed=4 * rows * depth, transcendentals=0
        ),
    )(*in_vmem(pieces), b_high, b_low)


def choose_kernel(which_ref, *refs):
    for i, value in enumerate(refs[:-1]):

        @pl.when(which_ref[0] == i)
        def _():
            refs[-1][...] = value[...]


def choose(which, values):
    return pl.pallas_call(
        choose_kernel,
        in_specs=[pl.BlockSpec(memory_space=pltpu.SMEM)] + [VMEM] * len(values),
        out_specs=VMEM,
        out_shape=pltpu.VMEM(values[0].shape, values[0].dtype),
        compiler_params=pltpu.CompilerParams(vmem_limit_bytes=4 << 20),
    )(which, *in_vmem(values))


def finish_kernel(col_ref, *refs):
    i, out = pl.program_id(0), refs[-1]
    at = pl.ds(i % 2 * out.shape[0], out.shape[0])
    early, late = refs[:3], refs[3:6]

    @pl.when(i < 2)
    def _():
        out[...] = early[0][at, :] + early[1][at, :] + early[2][at, :]

    @pl.when(i >= 2)
    def _():
        out[...] = late[0][at, :] + late[1][at, :] + late[2][at, :]


def finish(col, early, late):
    rows, width = early[0].shape
    return pl.pallas_call(
        finish_kernel,
        grid_spec=pltpu.PrefetchScalarGridSpec(
            num_scalar_prefetch=1,
            grid=(4,),
            in_specs=[VMEM] * 6,
            out_specs=pl.BlockSpec((rows // 2, width), lambda i, col: (i ^ col[0], 0)),
        ),
        out_shape=jax.ShapeDtypeStruct((2 * rows, width), jnp.float32),
        compiler_params=pltpu.CompilerParams(vmem_limit_bytes=8 << 20),
        name="finish",
    )(col, *in_vmem(early + late))


def after(values, anchors):
    return lax.optimization_barrier((tuple(values), tuple(anchors)))[0]


def per_device(left_factor, right_factor):
    rows, cols, layers = (lax.axis_size(name) for name in AXES)
    x, c, l = (lax.axis_index(name) for name in AXES)
    chunk = left_factor.shape[0] // layers
    quarter = chunk // cols

    def send(value, target):
        pairs = []
        for i in range(rows):
            for j in range(cols):
                for k in range(layers):
                    a, b, d = target(i, j, k)
                    pairs.append(((i * cols + j) * layers + k, (a * cols + b) * layers + d))
        return lax.ppermute(value, AXES, pairs)

    def over_y(i, j, k):
        return i, j ^ 2, k

    def over_core(i, j, k):
        return i, j ^ 1, k

    def take(layer, block):
        start = layer * chunk + block * quarter
        return lax.dynamic_slice_in_dim(left_factor, start, quarter, 0)

    source = lambda s: (((x + s) % rows) ^ c).reshape(1)
    step = jnp.where(c % 2 == 1, 1, rows - 1)
    scalars = (source(2), source(step), source(rows - step), source(0), c.reshape(1))
    taken = (take(l, c), take(l, c ^ 1), take(l, c ^ 2), take(l ^ 4, c ^ 3))
    scalars, taken, right_factor = lax.optimization_barrier((scalars, taken, right_factor))
    source2, source_p, source_q, source0, col = scalars

    b_high, b_low = prepare(right_factor)
    mul = lambda pieces: multiply(pieces, b_high, b_low)

    spread = [
        taken[0],
        send(taken[1], over_core),
        send(taken[2], over_y),
        send(taken[3], lambda i, j, k: (i, j ^ 3, k ^ 4)),
    ]

    def forward(i, j, k):
        return (i + (-1 if j % 2 else 1)) % rows, j, k

    def backward(i, j, k):
        return (i + (1 if j % 2 else -1)) % rows, j, k

    mine2 = send(choose(source2, spread), lambda i, j, k: ((i + 2) % rows, j, k))
    mine_p = send(choose(source_p, spread), backward)
    mine_q = send(choose(source_q, spread), forward)
    mine0 = choose(source0, spread)
    across0 = send(mine0, over_y)
    across2 = send(mine2, over_y)
    near2 = send(mine2, over_core)
    (opposite_e,) = mul([mine2, near2])
    first_e = send(opposite_e, forward)

    mine_p, mine_q, _ = after((mine_p, mine_q, mine2), (opposite_e,))
    across_p = send(mine_p, over_y)
    across_q = send(mine_q, over_y)
    near_p = send(mine_q, over_core)
    near_q = send(mine_p, over_core)
    p_e, q_e = mul([mine_p, near_p, mine_q, near_q])
    from_q_e = send(q_e, backward)
    from_p_e = send(p_e + first_e, forward)

    (across2,) = after((across2,), (p_e,))
    far2 = send(across2, over_core)
    (opposite_l,) = mul([across2, far2])
    first_l = send(opposite_l, forward)

    across_p, across_q = after((across_p, across_q), (opposite_l,))
    far_p = send(across_q, over_core)
    far_q = send(across_p, over_core)
    p_l, q_l = mul([across_p, far_p, across_q, far_q])
    from_q_l = send(q_l, backward)

    mine0, across0 = after((mine0, across0), (p_l,))
    near0 = send(mine0, over_core)
    far0 = send(across0, over_core)
    own_e, own_l = mul([mine0, near0, across0, far0])
    from_p_l = send(p_l + first_l, forward)

    return finish(col, [own_e, from_q_e, from_p_e], [own_l, from_q_l, from_p_l])


def solution(mesh):
    placed = (P("row", "col"), P("row", "col"))

    return jax.shard_map(
        per_device,
        mesh=mesh,
        in_specs=placed,
        out_specs=P(("row", "layer"), "col"),
        check_vma=False,
    )
```

```python
import functools

import jax
import jax.numpy as jnp
from jax import lax
from jax.experimental import pallas as pl
from jax.experimental.pallas import tpu as pltpu
from jax.sharding import PartitionSpec as P


AXES = ("row", "col", "layer")
BLOCK = 256
VMEM = pl.BlockSpec(memory_space=pltpu.VMEM)


def split(value):
    high = value.astype(jnp.bfloat16)
    return high, (value - high.astype(jnp.float32)).astype(jnp.bfloat16)


def prepare_kernel(b_ref, high_ref, low_ref):
    size = b_ref.shape[0]
    at = pl.ds(pl.program_id(0) * size, size)
    high_ref[at, :], low_ref[at, :] = split(b_ref[...])


def prepare(b):
    depth, width = b.shape
    return pl.pallas_call(
        prepare_kernel,
        grid=(depth // BLOCK,),
        in_specs=[pl.BlockSpec((BLOCK, width), lambda i: (i, 0))],
        out_specs=[VMEM, VMEM],
        out_shape=[pltpu.VMEM(b.shape, jnp.bfloat16)] * 2,
        compiler_params=pltpu.CompilerParams(vmem_limit_bytes=16 << 20),
        name="prepare",
    )(pltpu.with_memory_space_constraint(b, pltpu.HBM))


def hold_kernel(in_ref, out_ref):
    out_ref[0] = in_ref[0]


def hold(value):
    smem = pl.BlockSpec(memory_space=pltpu.SMEM)
    return pl.pallas_call(
        hold_kernel,
        in_specs=[smem],
        out_specs=smem,
        out_shape=jax.ShapeDtypeStruct(value.shape, value.dtype),
        compiler_params=pltpu.CompilerParams(vmem_limit_bytes=1 << 20),
        name="hold",
    )(value)


def multiply_kernel(count, *refs):
    pieces, (b_high, b_low), outs = refs[:count], refs[count : count + 2], refs[count + 2 :]
    high, low = split(jnp.concatenate([piece[...] for piece in pieces], 0))
    dot = functools.partial(jnp.dot, preferred_element_type=jnp.float32)
    size = outs[0].shape[0]
    for start in range(0, b_high.shape[1], BLOCK):
        at = slice(start, start + BLOCK)
        result = dot(high, b_high[:, at]) + dot(high, b_low[:, at]) + dot(low, b_high[:, at])
        for i, out in enumerate(outs):
            out[:, at] = result[i * size : (i + 1) * size]


def in_vmem(values):
    return [pltpu.with_memory_space_constraint(v, pltpu.VMEM) for v in values]


def multiply(pieces, split_b):
    (size, depth), width = pieces[0].shape, split_b[0].shape[1]
    rows, results = size * len(pieces), len(pieces) // 2
    return pl.pallas_call(
        functools.partial(multiply_kernel, len(pieces)),
        in_specs=[VMEM] * (len(pieces) + 2),
        out_specs=[VMEM] * results,
        out_shape=[pltpu.VMEM((2 * size, width), jnp.float32)] * results,
        compiler_params=pltpu.CompilerParams(vmem_limit_bytes=16 << 20),
        cost_estimate=pl.CostEstimate(
            flops=6 * rows * depth * width, bytes_accessed=4 * rows * depth, transcendentals=0
        ),
    )(*in_vmem(pieces), *split_b)


def choose_kernel(which_ref, *refs):
    for i, value in enumerate(refs[:-1]):

        @pl.when(which_ref[0] == i)
        def _():
            refs[-1][...] = value[...]


def choose(which, values):
    return pl.pallas_call(
        choose_kernel,
        in_specs=[pl.BlockSpec(memory_space=pltpu.SMEM)] + [VMEM] * len(values),
        out_specs=VMEM,
        out_shape=pltpu.VMEM(values[0].shape, values[0].dtype),
        compiler_params=pltpu.CompilerParams(vmem_limit_bytes=4 << 20),
    )(which, *in_vmem(values))


def finish_kernel(col_ref, *refs):
    out = refs[-1]
    at = pl.ds(pl.program_id(0) * out.shape[0], out.shape[0])
    out[...] = refs[0][at, :] + refs[1][at, :] + refs[2][at, :]


def finish(part, col, values, into=None):
    rows, width = values[0].shape
    given = () if into is None else (into,)
    return pl.pallas_call(
        finish_kernel,
        grid_spec=pltpu.PrefetchScalarGridSpec(
            num_scalar_prefetch=1,
            grid=(2,),
            in_specs=[VMEM] * 3 + [pl.BlockSpec(memory_space=pl.ANY)] * len(given),
            out_specs=pl.BlockSpec((rows // 2, width), lambda i, col: ((i + 2 * part) ^ col[0], 0)),
        ),
        out_shape=jax.ShapeDtypeStruct((2 * rows, width), jnp.float32),
        input_output_aliases={4: 0} if given else {},
        compiler_params=pltpu.CompilerParams(vmem_limit_bytes=8 << 20),
    )(col, *in_vmem(values), *given)


def after(values, anchors):
    return lax.optimization_barrier((tuple(values), tuple(anchors)))[0]


def per_device(left_factor, right_factor):
    rows, cols, layers = (lax.axis_size(name) for name in AXES)
    x, c, l = (lax.axis_index(name) for name in AXES)
    chunk = left_factor.shape[0] // layers
    quarter = chunk // cols

    def send(value, target):
        pairs = []
        for i in range(rows):
            for j in range(cols):
                for k in range(layers):
                    a, b, d = target(i, j, k)
                    pairs.append(((i * cols + j) * layers + k, (a * cols + b) * layers + d))
        return lax.ppermute(value, AXES, pairs)

    def over_y(i, j, k):
        return i, j ^ 2, k

    def over_core(i, j, k):
        return i, j ^ 1, k

    def take(layer, block):
        start = layer * chunk + block * quarter
        return lax.dynamic_slice_in_dim(left_factor, start, quarter, 0)

    source = lambda s: (((x + s) % rows) ^ c).reshape(1)
    step = jnp.where(c % 2 == 1, 1, rows - 1)
    scalars = (source(2), source(step), source(rows - step), source(0), c.reshape(1))
    taken = (take(l, c), take(l, c ^ 1), take(l, c ^ 2), take(l ^ 4, c ^ 3))
    scalars, taken, right_factor = lax.optimization_barrier((scalars, taken, right_factor))
    source2, source_p, source_q, source0, col = scalars

    split_b = prepare(right_factor)
    mul = lambda pieces: multiply(pieces, split_b)

    spread = [
        taken[0],
        send(taken[1], over_core),
        send(taken[2], over_y),
        send(taken[3], lambda i, j, k: (i, j ^ 3, k ^ 4)),
    ]

    def forward(i, j, k):
        return (i + (-1 if j % 2 else 1)) % rows, j, k

    def backward(i, j, k):
        return (i + (1 if j % 2 else -1)) % rows, j, k

    mine2 = send(choose(source2, spread), lambda i, j, k: ((i + 2) % rows, j, k))
    mine_p = send(choose(source_p, spread), backward)
    mine_q = send(choose(source_q, spread), forward)
    mine0 = choose(source0, spread)
    across0 = send(mine0, over_y)
    across2 = send(mine2, over_y)
    near2 = send(mine2, over_core)
    (opposite_e,) = mul([mine2, near2])
    first_e = send(opposite_e, forward)

    mine_p, mine_q, _ = after((mine_p, mine_q, mine2), (opposite_e,))
    across_p = send(mine_p, over_y)
    across_q = send(mine_q, over_y)
    near_p = send(mine_q, over_core)
    near_q = send(mine_p, over_core)
    p_e, q_e = mul([mine_p, near_p, mine_q, near_q])
    from_q_e = send(q_e, backward)
    from_p_e = send(p_e + first_e, forward)

    (across2,) = after((across2,), (p_e,))
    far2 = send(across2, over_core)
    (opposite_l,) = mul([across2, far2])
    first_l = send(opposite_l, forward)

    across_p, across_q = after((across_p, across_q), (opposite_l,))
    far_p = send(across_q, over_core)
    far_q = send(across_p, over_core)
    p_l, q_l = mul([across_p, far_p, across_q, far_q])
    from_q_l = send(q_l, backward)

    mine0, across0 = after((mine0, across0), (p_l,))
    near0 = send(mine0, over_core)
    far0 = send(across0, over_core)
    own_e, own_l = mul([mine0, near0, across0, far0])
    from_p_l = send(p_l + first_l, forward)

    result = finish(0, hold(col), [own_e, from_q_e, from_p_e])
    return finish(1, col, [own_l, from_q_l, from_p_l], result)


def solution(mesh):
    placed = (P("row", "col"), P("row", "col"))

    return jax.shard_map(
        per_device,
        mesh=mesh,
        in_specs=placed,
        out_specs=P(("row", "layer"), "col"),
        check_vma=False,
    )
```
